32 devices in a mesh: rep: 4 (over y, core), tp: 8 (over z, x).
Axes of the slice: x: 2, y: 2, z: 4, core: 2. Of those that a mesh axis runs over, the one named last changes fastest.
Arguments:
- activations: bfloat16 [4, 2048, 4096], P('rep', 'tp'), may hold values from -6 to 6
- cotangent: bfloat16 [4, 2048, 8192], P('rep', None, 'tp'), may hold values from -0.13183594 to 0.13183594
- drift: bfloat16 [4, 4096, 8192], P('rep', None, 'tp'), may hold values from -8 to 8
- outer_weights: float32 [4096, 8192], P(('rep', 'tp')), may hold values from -6 to 6
- momentum: float32 [4096, 8192], P(('rep', 'tp')), may hold values from -6 to 6
Outputs:
- weights: bfloat16 [4096, 8192], P(None, 'tp')
- new_outer: float32 [4096, 8192], P(('rep', 'tp'))
- new_momentum: float32 [4096, 8192], P(('rep', 'tp'))
The draws below stay inside these ranges and needn't reach their ends.
All inputs are finite; a program needn't handle non-finite values.
Results may differ from the reference program's by a relative error of at most 0.0085.
Values may be sent and summed in bfloat16 or wider, within the bound.
No kernel may reach another device: no remote copies, remote signals or barrier semaphores. Data moves between devices by JAX's collectives and lax.ppermute only.
A program may use at most 128 MiB of HBM per device.

```python
import jax
import jax.numpy as jnp
from jax import lax

D = 4096
FFW = 8192
TOK = 2048
REPS = 4
N_REP = 4


def strengthened(drawn, rng, source, target, blocks, factor):
    def block_of(position):
        return (jnp.arange(drawn.shape[position]) // (drawn.shape[position] // blocks)).reshape((-1,) + (1,) * (drawn.ndim - 1 - position))

    near = jax.random.permutation(rng, blocks)[block_of(target)]
    second = (block_of(target) + blocks // 2) % blocks
    return jnp.where((block_of(source) == near) | (block_of(source) == second), factor * drawn, drawn)


def steps_of(key, dims, cuts, least, largest):
    def one(dim, parts):
        heights = jax.random.uniform(jax.random.fold_in(jax.random.fold_in(key, 6), dim), (parts,), jnp.float32, least / len(cuts), largest / len(cuts))
        return jnp.repeat(jnp.exp(heights), dims[dim] // parts).reshape((-1,) + (1,) * (len(dims) - dim - 1))

    factor_of = one(*cuts[0])
    for cut in cuts[1:]:
        factor_of = factor_of * one(*cut)
    return factor_of


def normal_values(key, extent, spread, most, pieces=(), held_as=jnp.bfloat16):
    values = jax.random.normal(key, extent, jnp.float32) * spread
    if len(pieces) > 0:
        values = steps_of(key, extent, pieces, -0.22, 0.18) * values
    return jnp.clip(values, min=-most, max=most).astype(held_as)


def noise_with(stream_key, shape, scale, bound, split, heavy, dtype=jnp.bfloat16):
    entries = scale * jax.random.normal(stream_key, shape, jnp.float32)
    if split:
        entries = entries * steps_of(stream_key, shape, split, -0.22, 0.18)
    return jnp.clip(strengthened(entries, jax.random.fold_in(stream_key, 3), *heavy), -bound, bound).astype(dtype)


def setup_inputs(seed: int = 0) -> dict:
    streams_of = jax.random.split(jax.random.key(seed), 6)
    activations = normal_values(streams_of[0], (REPS, TOK, D), 1.0, 6.0, ((0, 4), (1, 8)))
    cotangent = normal_values(streams_of[1], (REPS, TOK, FFW), (TOK ** -0.5), 0.13183594, ((0, 4), (2, 8)))
    drift = noise_with(streams_of[2], (REPS, D, FFW), 1.0, 8.0, ((0, 4), (2, 8)), (0, 1, 4, 2.0))
    outer_weights = normal_values(streams_of[3], (D, FFW), 1.0, 6.0, ((0, 32),), jnp.float32)
    momentum = normal_values(streams_of[4], (D, FFW), 1.0, 6.0, ((0, 32),), jnp.float32)
    return dict(activations=activations, cotangent=cotangent, drift=drift, outer_weights=outer_weights, momentum=momentum)


outer_rate = 0.7
nesterov = 0.9


def reference(activations, cotangent, drift, outer_weights, momentum):
    def per_group(total, items):
        acts, cot, own = items
        grad = jnp.dot(acts.T, cot, preferred_element_type=jnp.float32)
        delta = lax.optimization_barrier((own.astype(jnp.float32) + grad).astype(jnp.bfloat16))
        return total + delta.astype(jnp.float32), None

    start = jnp.zeros((drift.shape[1], drift.shape[2]), jnp.float32)
    summed, _ = lax.scan(per_group, start, (activations, cotangent, drift))
    average = summed / N_REP
    new_momentum = nesterov * momentum + average
    new_outer = outer_weights - outer_rate * (average + nesterov * new_momentum)
    weights = new_outer.astype(jnp.bfloat16)
    return weights, new_outer, new_momentum
```

```python
import jax
import jax.numpy as jnp
from jax import lax
from jax.sharding import PartitionSpec as P

outer_rate = 0.7
nesterov = 0.9


def on_device(activations, cotangent, drift, outer_weights, momentum):
    replicas = lax.axis_size("rep")
    cot_rows = cotangent[0]
    grad = jnp.einsum(
        "td,tf->df",
        lax.all_gather(activations, "tp", axis=1, tiled=True)[0],
        cot_rows,
        preferred_element_type=jnp.float32,
    )
    delta = lax.optimization_barrier((drift[0].astype(jnp.float32) + grad).astype(jnp.bfloat16))
    summed = lax.psum_scatter(
        delta.astype(jnp.float32).astype(jnp.bfloat16), "rep", scatter_dimension=0, tiled=True
    ).astype(jnp.float32)
    summed = lax.all_to_all(
        summed.astype(jnp.bfloat16), "tp", split_axis=0, concat_axis=1, tiled=True
    ).astype(summed.dtype)
    average = summed / replicas
    new_momentum = nesterov * momentum + average
    new_outer = outer_weights - outer_rate * (average + nesterov * new_momentum)
    rounded = new_outer.astype(jnp.bfloat16)
    spread = lax.all_to_all(rounded, "tp", split_axis=1, concat_axis=0, tiled=True)
    weights = lax.all_gather(spread, "rep", axis=0, tiled=True)
    return (weights, new_outer, new_momentum)


def solution(mesh):
    in_specs = (
        P("rep", "tp", None),
        P("rep", None, "tp"),
        P("rep", None, "tp"),
        P(("rep", "tp"), None),
        P(("rep", "tp"), None),
    )
    out_specs = (P(None, "tp"), P(("rep", "tp"), None), P(("rep", "tp"), None))
    return jax.shard_map(
        on_device, mesh=mesh, in_specs=in_specs, out_specs=out_specs, check_vma=False
    )
```

```python
import functools
import math

import jax
import jax.numpy as jnp
from jax import lax
from jax.experimental import pallas as pl
from jax.experimental.pallas import tpu as pltpu
from jax.sharding import PartitionSpec as P


outer_rate = 0.7
nesterov = 0.9


def cut(rows):
    if rows % 128:
        return ((0, rows),)
    unit = rows // 4
    return ((2 * unit, unit), (0, 2 * unit), (3 * unit, unit))


f32, bf16 = jnp.float32, jnp.bfloat16


def sort_kernel(inner, outer, rows, strips, at_ref, acts_ref, *refs):
    out_refs, masks = refs[: inner * len(strips)], refs[inner * len(strips) :]
    span = acts_ref.shape[1]

    if not masks:
        to = lax.broadcasted_iota(jnp.int32, (rows, rows), 0)
        same = jnp.where(to == lax.broadcasted_iota(jnp.int32, (rows, rows), 1), 1.0, 0.0).astype(bf16)
        for k in range(inner):
            for i in range(outer):
                start = pl.multiple_of((i * inner + lax.rem(at_ref[0] + k, inner)) * rows, rows)
                turned = lax.dot_general(
                    same, acts_ref[:, pl.ds(start, rows)], (((1,), (1,)), ((), ())), preferred_element_type=f32
                ).astype(bf16)
                for q, (low, strip) in enumerate(strips):
                    out_refs[k * len(strips) + q][i * strip : (i + 1) * strip] = turned[low : low + strip]
        return

    @pl.when(pl.program_id(0) == 0)
    def _():
        for q, (low, strip) in enumerate(strips):
            m = outer * strip
            to = lax.broadcasted_iota(jnp.int32, (m, span), 0)
            source = lax.broadcasted_iota(jnp.int32, (m, span), 1)
            base = lax.shift_right_logical(to, strip.bit_length() - 1) * (inner * rows) + (to & (strip - 1)) + low
            for k in range(inner):
                column = lax.rem(at_ref[0] + k, inner) * rows
                masks[k * len(strips) + q][...] = jnp.where(source == base + column, 1.0, 0.0).astype(bf16)

    for mask, out_ref in zip(masks, out_refs):
        out_ref[...] = lax.dot_general(
            mask[...], acts_ref[...], (((1,), (1,)), ((), ())), preferred_element_type=f32
        ).astype(bf16)


def sort_columns(acts, at, inner, outer, rows, strips):
    tokens, width = acts.shape
    reps = at.shape[0] - 1
    span = width // reps
    return pl.pallas_call(
        functools.partial(sort_kernel, inner, outer, rows, strips),
        grid_spec=pltpu.PrefetchScalarGridSpec(
            num_scalar_prefetch=1,
            grid=(reps,),
            in_specs=[pl.BlockSpec((tokens, span), lambda j, at: (0, at[1 + j]))],
            out_specs=[pl.BlockSpec((outer * size, tokens), lambda j, at: (j, 0)) for _ in range(inner) for _, size in strips],
            scratch_shapes=[pltpu.VMEM((outer * size, span), bf16) for _ in range(inner) for _, size in strips if rows % 128],
        ),
        out_shape=[jax.ShapeDtypeStruct((reps * outer * size, tokens), bf16) for _ in range(inner) for _, size in strips],
        cost_estimate=pl.CostEstimate(flops=2 * tokens * width * span, bytes_accessed=4 * tokens * width, transcendentals=0),
    )(at, acts)


def dot_kernel(outer, inner, count, at_ref, *refs):
    blocks, cots = refs[: outer * inner], refs[outer * inner : outer * inner + count]
    away_ref, here_ref = refs[-2:]
    depth = blocks[0].shape[1]
    half = away_ref.shape[0]
    for i in range(count):

        @pl.when(pl.program_id(0) == i)
        def _(i=i):
            total = None
            for s in range(outer):
                for k in range(inner):
                    owner = lax.rem(at_ref[1] + (outer - s), outer) * inner + lax.rem(at_ref[0] + (inner - k), inner)
                    start = pl.multiple_of(owner * depth, depth)
                    term = jnp.dot(blocks[s * inner + k][...], cots[i][pl.ds(start, depth), :], preferred_element_type=f32)
                    total = term if total is None else total + term
            here_ref[...] = total[:half]
            away_ref[...] = total[half:].astype(away_ref.dtype)


def partial_grad(blocks, cots, at, outer, first=0, held=()):
    count = len(cots)
    inner = len(blocks) // outer
    m, depth = blocks[0].shape
    tokens, cols = cots[0].shape
    tile = min(cols, 512)
    tiles = cols // tile

    def cot_spec(k):
        return pl.BlockSpec((tokens, tile), lambda i, j, at: (0, jnp.where(i == k, j, jnp.where(i < k, 0, tiles - 1))))

    out = pl.BlockSpec((m // 2, tile), lambda i, j, at: (0, lax.rem(at[0] + (2 * inner - first - i), inner) * tiles + j))
    return pl.pallas_call(
        functools.partial(dot_kernel, outer, inner, count),
        grid_spec=pltpu.PrefetchScalarGridSpec(
            num_scalar_prefetch=1,
            grid=(count, tiles),
            in_specs=[pl.BlockSpec((m, depth), lambda i, j, at: (0, 0)) for _ in blocks]
            + [cot_spec(k) for k in range(count)]
            + [pl.BlockSpec(memory_space=pl.ANY) for _ in held],
            out_specs=[out, out],
        ),
        out_shape=[jax.ShapeDtypeStruct((m // 2, inner * cols), d) for d in (bf16, f32)],
        input_output_aliases={1 + len(blocks) + count + i: i for i in range(len(held))},
        cost_estimate=pl.CostEstimate(
            flops=2 * m * tokens * count * cols, bytes_accessed=2 * (m * tokens + tokens * count * cols + 2 * m * count * cols), transcendentals=0
        ),
    )(at, *blocks, *cots, *held)


def step_kernel(outer, reps, at_ref, *refs):
    parts, (weights_ref, momentum_ref) = refs[:outer], refs[outer : outer + 2]
    new_weights_ref, new_momentum_ref, *rounded = refs[-2 - outer :]
    for k in range(outer):

        @pl.when(pl.program_id(0) == k)
        def _(k=k):
            average = parts[k][...].astype(f32) / reps
            new_momentum = nesterov * momentum_ref[...] + average
            new_weights = weights_ref[...] - outer_rate * (average + nesterov * new_momentum)
            new_momentum_ref[...] = new_momentum
            new_weights_ref[...] = new_weights
            rounded[k][...] = new_weights.astype(bf16)


def outer_step(parts, weights, momentum, held, at, low, reps):
    outer = len(parts)
    strip, span = parts[0].shape
    small = pl.BlockSpec((strip, span), lambda k, at: (0, 0))
    state = pl.BlockSpec((strip, span), lambda k, at: (low // strip, lax.rem(at[1] + (outer - k), outer)))
    shape = jax.ShapeDtypeStruct(weights.shape, f32)
    out = pl.pallas_call(
        functools.partial(step_kernel, outer, reps),
        grid_spec=pltpu.PrefetchScalarGridSpec(
            num_scalar_prefetch=1,
            grid=(outer,),
            in_specs=[small] * outer + [state, state] + [pl.BlockSpec(memory_space=pl.ANY)] * len(held),
            out_specs=[state, state] + [small] * outer,
        ),
        out_shape=[shape, shape] + [jax.ShapeDtypeStruct((strip, span), bf16)] * outer,
        input_output_aliases={outer + 3 + i: i for i in range(len(held))},
        cost_estimate=pl.CostEstimate(flops=8 * outer * strip * span, bytes_accessed=20 * outer * strip * span, transcendentals=0),
    )(at, *parts, weights, momentum, *held)
    return out[:2], out[2:]


def spread_kernel(outer, inner, at_ref, *refs):
    ins, outs = refs[: outer * inner], refs[outer * inner :]
    for k in range(outer):
        index = lax.rem(at_ref[1] + (outer - k), outer)
        for j in range(inner):
            outs[j][index] = ins[k * inner + j][...]


def spread(parts, at, inner):
    outer = len(parts)
    strip, span = parts[0].shape
    cols = span // inner

    def column(j):
        return pl.BlockSpec((strip, cols), lambda i, at: (0, lax.rem(at[0] + j, inner)))

    return pl.pallas_call(
        functools.partial(spread_kernel, outer, inner),
        grid_spec=pltpu.PrefetchScalarGridSpec(
            num_scalar_prefetch=1,
            grid=(1,),
            in_specs=[column(j) for _ in range(outer) for j in range(inner)],
            out_specs=[pl.BlockSpec((outer, strip, cols), lambda i, at: (0, 0, 0))] * inner,
        ),
        out_shape=[jax.ShapeDtypeStruct((outer, strip, cols), bf16)] * inner,
        cost_estimate=pl.CostEstimate(flops=0, bytes_accessed=4 * outer * strip * span, transcendentals=0),
    )(at, *[p for p in parts for _ in range(inner)])


def write_kernel(count, low, at_ref, *refs):
    out_ref, sems = refs[-2:]
    strip = refs[0].shape[1]
    copies = []
    for i in range(count):
        target = out_ref.at[at_ref[3 * i], at_ref[3 * i + 1], :, at_ref[3 * i + 2], pl.ds(low, strip), :]
        copies.append(pltpu.make_async_copy(refs[i], target, sems.at[i]))
        copies[-1].start()
    for copy in copies:
        copy.wait()


def write(found, at, held, shape, low):
    small = pl.BlockSpec(found[0].shape, lambda i, at: (0, 0, 0))
    more = [] if held is None else [held]
    return pl.pallas_call(
        functools.partial(write_kernel, len(found), low),
        grid_spec=pltpu.PrefetchScalarGridSpec(
            num_scalar_prefetch=1,
            grid=(1,),
            in_specs=[small] * len(found) + [pl.BlockSpec(memory_space=pl.ANY) for _ in more],
            out_specs=pl.BlockSpec(memory_space=pltpu.HBM),
            scratch_shapes=[pltpu.SemaphoreType.DMA((len(found),))],
        ),
        out_shape=jax.ShapeDtypeStruct(shape, bf16),
        input_output_aliases={1 + len(found) + i: i for i in range(len(more))},
        cost_estimate=pl.CostEstimate(flops=0, bytes_accessed=4 * len(found) * found[0].size, transcendentals=0),
    )(at, *found, *more)


def add_kernel(high, here_ref, away_ref, *out_refs):
    for j in range(1, high):

        @pl.when(pl.program_id(0) == j - 1)
        def _(j=j):
            out_refs[j - 1][...] = (here_ref[...] + away_ref[...].astype(f32)).astype(bf16)


def chip_sum(here, away, high):
    m, width = here.shape
    block = pl.BlockSpec((m // high, width // 2), lambda j, i: (j + 1, i))
    return pl.pallas_call(
        functools.partial(add_kernel, high),
        grid=(high - 1, 2),
        in_specs=[block, block],
        out_specs=[
            pl.BlockSpec((m // high, width // 2), lambda j, i, k=k: (0, jnp.where(j == k, i, jnp.where(j < k, 0, 1)))) for k in range(high - 1)
        ],
        out_shape=[jax.ShapeDtypeStruct((m // high, width), bf16) for _ in range(high - 1)],
        cost_estimate=pl.CostEstimate(flops=m * width, bytes_accessed=8 * m * width * (high - 1) // high, transcendentals=0),
    )(here, away)


def total_kernel(outer, inner, strip, at_ref, here_ref, away_ref, *refs):
    outs = refs[-outer:]
    drifts = refs[-outer - inner : -outer]
    got = refs[: -outer - inner]
    cols = here_ref.shape[1] // inner
    for k in range(outer):
        index = lax.rem(at_ref[1] + k, outer)
        at_rows = pl.ds(pl.multiple_of(index * strip, strip), strip)
        for j in range(inner):
            at_cols = pl.ds(pl.multiple_of(lax.rem(at_ref[0] + (inner - j), inner) * cols, cols), cols)
            total = here_ref[at_rows, at_cols] + away_ref[at_rows, at_cols].astype(f32) + drifts[j][index].astype(f32)
            for ref in got:
                total = total + ref[at_rows, at_cols].astype(f32)
            outs[k][:, at_cols] = total.astype(bf16)


def full_sum(here, away, got, drifts, at, outer, low, strip):
    inner = len(drifts)
    cols = drifts[0].shape[2]
    span = inner * cols
    rows = pl.BlockSpec((outer * strip, span), lambda i, at: (0, 0))
    return pl.pallas_call(
        functools.partial(total_kernel, outer, inner, strip),
        grid_spec=pltpu.PrefetchScalarGridSpec(
            num_scalar_prefetch=1,
            grid=(1,),
            in_specs=[rows] * (2 + len(got)) + [pl.BlockSpec((outer, strip, cols), lambda i, at: (0, low // strip, 0)) for _ in drifts],
            out_specs=[pl.BlockSpec((strip, span), lambda i, at: (0, 0))] * outer,
        ),
        out_shape=[jax.ShapeDtypeStruct((strip, span), bf16)] * outer,
        cost_estimate=pl.CostEstimate(flops=4 * outer * strip * span, bytes_accessed=12 * outer * strip * span, transcendentals=0),
    )(at, here, away, *got, *drifts)


def take_kernel(at_ref, in_ref, out_ref):
    out_ref[...] = in_ref[...]


def take(array, at, count):
    _, rows, cols = array.shape
    return pl.pallas_call(
        take_kernel,
        grid_spec=pltpu.PrefetchScalarGridSpec(
            num_scalar_prefetch=1,
            grid=(count, 2),
            in_specs=[pl.BlockSpec((1, rows // 2, cols), lambda j, i, at: (at[j], i, 0))],
            out_specs=pl.BlockSpec((1, rows // 2, cols), lambda j, i, at: (j, i, 0)),
        ),
        out_shape=jax.ShapeDtypeStruct((count, rows, cols), array.dtype),
        cost_estimate=pl.CostEstimate(flops=0, bytes_accessed=4 * count * rows * cols, transcendentals=0),
    )(at, array)


def twin_kernel(count, at_ref, mine_ref, got_ref, *out_refs):
    for j in range(count):

        @pl.when(pl.program_id(0) == j)
        def _(j=j):
            out_refs[j][...] = (mine_ref[0].astype(f32) + got_ref[0].astype(f32)).astype(bf16)


def twin_sum(mine, got, at):
    count, rows, cols = got.shape
    count -= 1
    return pl.pallas_call(
        functools.partial(twin_kernel, count),
        grid_spec=pltpu.PrefetchScalarGridSpec(
            num_scalar_prefetch=1,
            grid=(count, 2),
            in_specs=[
                pl.BlockSpec((1, rows // 2, cols), lambda j, i, at: (at[j + 1], i, 0)),
                pl.BlockSpec((1, rows // 2, cols), lambda j, i, at: (j + 1, i, 0)),
            ],
            out_specs=[
                pl.BlockSpec((rows // 2, cols), lambda j, i, at, k=k: (jnp.where(j == k, i, jnp.where(j < k, 0, 1)), 0)) for k in range(count)
            ],
        ),
        out_shape=[jax.ShapeDtypeStruct((rows, cols), bf16) for _ in range(count)],
        cost_estimate=pl.CostEstimate(flops=count * rows * cols, bytes_accessed=6 * count * rows * cols, transcendentals=0),
    )(at, mine, got)


def drift_kernel(inner, at_ref, *refs):
    outs, ins = refs[-inner:], refs[:-inner]
    total = ins[0][0].astype(f32) + ins[1][0].astype(f32)
    for ref in ins[2:]:
        total = total + ref[...].astype(f32)
    for j in range(inner):

        @pl.when(pl.program_id(0) == j)
        def _(j=j):
            outs[j][0] = total.astype(bf16)


def drift_sum(mine, got, more, at, place, inner, outer):
    _, length, cols = mine.shape
    rows = length // (inner * outer)

    def part(j, i, ref):
        return i * inner + lax.rem(ref[0] + j, inner)

    return pl.pallas_call(
        functools.partial(drift_kernel, inner),
        grid_spec=pltpu.PrefetchScalarGridSpec(
            num_scalar_prefetch=1,
            grid=(inner, outer),
            in_specs=[
                pl.BlockSpec((1, rows, cols), lambda j, i, ref: (ref[2], part(j, i, ref), 0)),
                pl.BlockSpec((1, rows, cols), lambda j, i, ref: (0, part(j, i, ref), 0)),
            ]
            + [pl.BlockSpec((rows, cols), lambda j, i, ref: (part(j, i, ref), 0)) for _ in more],
            out_specs=[
                pl.BlockSpec((1, rows, cols), lambda j, i, ref, k=k: (jnp.where(j == k, i, jnp.where(j < k, 0, outer - 1)), 0, 0))
                for k in range(inner)
            ],
        ),
        out_shape=[jax.ShapeDtypeStruct((outer, rows, cols), bf16) for _ in range(inner)],
        cost_estimate=pl.CostEstimate(flops=3 * length * cols, bytes_accessed=8 * length * cols, transcendentals=0),
    )(jnp.concatenate([place, at[:1]]), mine, got, *more)


def on_device(activations, cotangent, drift, outer_weights, momentum):
    reps, tps = lax.axis_size("rep"), lax.axis_size("tp")
    inner = 2 ** (int(math.log2(tps)) // 2)
    outer = tps // inner
    pair = 2
    high = reps // pair
    rep, tp = lax.axis_index("rep"), lax.axis_index("tp")
    z, x = lax.div(tp, inner), lax.rem(tp, inner)
    y, c = lax.div(rep, pair), lax.rem(rep, pair)

    def over_x(v, k):
        return lax.ppermute(v, "tp", [(a * inner + b, a * inner + (b + k) % inner) for a in range(outer) for b in range(inner)])

    def over_z(v, k):
        return lax.ppermute(v, "tp", [(a * inner + b, (a + k) % outer * inner + b) for a in range(outer) for b in range(inner)])

    def over_y(v, k):
        return lax.ppermute(v, "rep", [(a * pair + b, (a + k) % high * pair + b) for a in range(high) for b in range(pair)])

    def over_c(v):
        return lax.ppermute(v, "rep", [(a, a ^ 1) for a in range(reps)])

    def ahead(index, k, n):
        return lax.rem(index + k, n)

    acts, cot = activations[0], cotangent[0]
    _, width = acts.shape
    cols = cot.shape[1]
    rows = outer_weights.shape[0]
    strips = cut(rows)
    n = len(strips)

    order = [ahead(y, jy, high) * pair + (c ^ jc) for jc in range(pair) for jy in range(high)]
    at = jnp.stack([x, *order]).astype(jnp.int32)
    place = jnp.stack([x, z]).astype(jnp.int32)
    own = sort_columns(acts, at, inner, outer, rows, strips)
    ring = [[own[q]] for q in range(n)]
    for q in range(n):
        for k in range(1, inner):
            ring[q].append(over_x(own[k * n + q], k))
    cots = [cot]
    for k in range(1, inner):
        cots.append(over_x(cot, k))
    for _ in range(1, outer):
        for q in range(n):
            for _ in range(inner):
                ring[q].append(over_z(ring[q][-inner], 1))

    mine = drift[0].reshape(reps, tps * rows, cols)
    near = jnp.stack(order[:high]).astype(jnp.int32)
    got = take(mine, near ^ 1, high)
    got = over_c(got)
    more = list(twin_sum(mine, got, near))
    for k in range(1, high):
        more[k - 1] = over_y(more[k - 1], k)
    drifts = list(drift_sum(mine, got, more, near, place, inner, outer))
    for k in range(1, inner):
        drifts[k] = over_x(drifts[k], k)

    weights, held = None, ()
    for q, (low, strip) in enumerate(strips):
        if q == 0:
            early = partial_grad(ring[q], cots[:1], place, outer)
            away, here = partial_grad(ring[q], cots[1:], place, outer, 1, early)
        else:
            away, here = partial_grad(ring[q], cots, place, outer)
        away = over_c(away)
        sent = chip_sum(here, away, high)
        got = []
        for j in range(1, high):
            got.append(over_y(sent[j - 1], j))
        parts = list(full_sum(here, away, got, drifts, place, outer, low, strip))
        for k in range(1, outer):
            parts[k] = over_z(parts[k], k)
        held, parts = outer_step(parts, outer_weights, momentum, held, place, low, reps)
        parts = list(parts)
        for k in range(1, outer):
            parts[k] = over_z(parts[k], outer - k)
        parts = list(spread(parts[:1] + parts[:0:-1], place, inner))
        for k in range(1, inner):
            parts[k] = over_x(parts[k], k)
        found, target = [], []
        for j in range(high):
            for k in range(inner):
                near = parts[k]
                if j > 0:
                    near = over_y(near, j)
                far = over_c(near)
                found += [near, far]
                for there in (c, c ^ 1):
                    target += [ahead(y, high - j, high), there, ahead(x, inner - k, inner)]
        weights = write(found, jnp.stack(target).astype(jnp.int32), weights, (high, pair, outer, inner, rows, cols), low)
    return (weights.reshape(width, cols), *held)


def solution(mesh):
    in_specs = (
        P("rep", "tp", None),
        P("rep", None, "tp"),
        P("rep", None, "tp"),
        P(("rep", "tp"), None),
        P(("rep", "tp"), None),
    )
    out_specs = (P(None, "tp"), P(("rep", "tp"), None), P(("rep", "tp"), None))

    return jax.shard_map(on_device, mesh=mesh, in_specs=in_specs, out_specs=out_specs, check_vma=False)
```

```python
import functools
import math

import jax
import jax.numpy as jnp
from jax import lax
from jax.experimental import pallas as pl
from jax.experimental.pallas import tpu as pltpu
from jax.sharding import PartitionSpec as P


outer_rate = 0.7
nesterov = 0.9


def cut(rows):
    if rows % 128:
        return ((0, rows),)
    unit = rows // 4
    return ((0, unit), (unit, unit), (2 * unit, unit), (3 * unit, unit))


f32, bf16 = jnp.float32, jnp.bfloat16


def sort_kernel(inner, outer, rows, strips, at_ref, acts_ref, *refs):
    out_refs, masks = refs[: inner * len(strips)], refs[inner * len(strips) :]
    span = acts_ref.shape[1]

    if not masks:
        to = lax.broadcasted_iota(jnp.int32, (rows, rows), 0)
        same = jnp.where(to == lax.broadcasted_iota(jnp.int32, (rows, rows), 1), 1.0, 0.0).astype(bf16)
        for k in range(inner):
            for i in range(outer):
                start = pl.multiple_of((i * inner + lax.rem(at_ref[0] + k, inner)) * rows, rows)
                turned = lax.dot_general(
                    same, acts_ref[:, pl.ds(start, rows)], (((1,), (1,)), ((), ())), preferred_element_type=f32
                ).astype(bf16)
                for q, (low, strip) in enumerate(strips):
                    out_refs[k * len(strips) + q][i * strip : (i + 1) * strip] = turned[low : low + strip]
        return

    @pl.when(pl.program_id(0) == 0)
    def _():
        for q, (low, strip) in enumerate(strips):
            m = outer * strip
            to = lax.broadcasted_iota(jnp.int32, (m, span), 0)
            source = lax.broadcasted_iota(jnp.int32, (m, span), 1)
            base = lax.shift_right_logical(to, strip.bit_length() - 1) * (inner * rows) + (to & (strip - 1)) + low
            for k in range(inner):
                column = lax.rem(at_ref[0] + k, inner) * rows
                masks[k * len(strips) + q][...] = jnp.where(source == base + column, 1.0, 0.0).astype(bf16)

    for mask, out_ref in zip(masks, out_refs):
        out_ref[...] = lax.dot_general(
            mask[...], acts_ref[...], (((1,), (1,)), ((), ())), preferred_element_type=f32
        ).astype(bf16)


def sort_columns(acts, at, inner, outer, rows, strips):
    tokens, width = acts.shape
    reps = at.shape[0] - 1
    span = width // reps
    return pl.pallas_call(
        functools.partial(sort_kernel, inner, outer, rows, strips),
        grid_spec=pltpu.PrefetchScalarGridSpec(
            num_scalar_prefetch=1,
            grid=(reps,),
            in_specs=[pl.BlockSpec((tokens, span), lambda j, at: (0, at[1 + j]))],
            out_specs=[pl.BlockSpec((outer * size, tokens), lambda j, at: (j, 0)) for _ in range(inner) for _, size in strips],
            scratch_shapes=[pltpu.VMEM((outer * size, span), bf16) for _ in range(inner) for _, size in strips if rows % 128],
        ),
        out_shape=[jax.ShapeDtypeStruct((reps * outer * size, tokens), bf16) for _ in range(inner) for _, size in strips],
        compiler_params=pltpu.CompilerParams(vmem_limit_bytes=24 << 20),
        cost_estimate=pl.CostEstimate(flops=2 * tokens * width * span, bytes_accessed=4 * tokens * width, transcendentals=0),
    )(at, acts)


def dot_kernel(outer, inner, count, at_ref, *refs):
    blocks, cots = refs[: outer * inner], refs[outer * inner : outer * inner + count]
    away_ref, here_ref = refs[-2:]
    depth = blocks[0].shape[1]
    half = away_ref.shape[0]
    for i in range(count):

        @pl.when(pl.program_id(0) == i)
        def _(i=i):
            total = None
            for s in range(outer):
                for k in range(inner):
                    owner = lax.rem(at_ref[1] + (outer - s), outer) * inner + lax.rem(at_ref[0] + (inner - k), inner)
                    start = pl.multiple_of(owner * depth, depth)
                    term = jnp.dot(blocks[s * inner + k][...], cots[i][pl.ds(start, depth), :], preferred_element_type=f32)
                    total = term if total is None else total + term
            here_ref[...] = total[:half]
            away_ref[...] = total[half:].astype(away_ref.dtype)


def partial_grad(blocks, cots, at, outer, first=0, held=()):
    count = len(cots)
    inner = len(blocks) // outer
    m, depth = blocks[0].shape
    tokens, cols = cots[0].shape
    tile = min(cols, 512)
    tiles = cols // tile

    def cot_spec(k):
        return pl.BlockSpec((tokens, tile), lambda i, j, at: (0, jnp.where(i == k, j, jnp.where(i < k, 0, tiles - 1))))

    out = pl.BlockSpec((m // 2, tile), lambda i, j, at: (0, lax.rem(at[0] + (2 * inner - first - i), inner) * tiles + j))
    return pl.pallas_call(
        functools.partial(dot_kernel, outer, inner, count),
        grid_spec=pltpu.PrefetchScalarGridSpec(
            num_scalar_prefetch=1,
            grid=(count, tiles),
            in_specs=[pl.BlockSpec((m, depth), lambda i, j, at: (0, 0)) for _ in blocks]
            + [cot_spec(k) for k in range(count)]
            + [pl.BlockSpec(memory_space=pl.ANY) for _ in held],
            out_specs=[out, out],
        ),
        out_shape=[jax.ShapeDtypeStruct((m // 2, inner * cols), d) for d in (bf16, f32)],
        input_output_aliases={1 + len(blocks) + count + i: i for i in range(len(held))},
        compiler_params=pltpu.CompilerParams(vmem_limit_bytes=24 << 20),
        cost_estimate=pl.CostEstimate(
            flops=2 * m * tokens * count * cols, bytes_accessed=2 * (m * tokens + tokens * count * cols + 2 * m * count * cols), transcendentals=0
        ),
    )(at, *blocks, *cots, *held)


def step_kernel(outer, reps, at_ref, *refs):
    parts, (weights_ref, momentum_ref) = refs[:outer], refs[outer : outer + 2]
    new_weights_ref, new_momentum_ref, *rounded = refs[-2 - outer :]
    for k in range(outer):

        @pl.when(pl.program_id(0) == k)
        def _(k=k):
            average = parts[k][...].astype(f32) / reps
            new_momentum = nesterov * momentum_ref[...] + average
            new_weights = weights_ref[...] - outer_rate * (average + nesterov * new_momentum)
            new_momentum_ref[...] = new_momentum
            new_weights_ref[...] = new_weights
            rounded[k][...] = new_weights.astype(bf16)


def outer_step(parts, weights, momentum, held, at, low, reps):
    outer = len(parts)
    strip, span = parts[0].shape
    small = pl.BlockSpec((strip, span), lambda k, at: (0, 0))
    state = pl.BlockSpec((strip, span), lambda k, at: (low // strip, lax.rem(at[1] + (outer - k), outer)))
    shape = jax.ShapeDtypeStruct(weights.shape, f32)
    out = pl.pallas_call(
        functools.partial(step_kernel, outer, reps),
        grid_spec=pltpu.PrefetchScalarGridSpec(
            num_scalar_prefetch=1,
            grid=(outer,),
            in_specs=[small] * outer + [state, state] + [pl.BlockSpec(memory_space=pl.ANY)] * len(held),
            out_specs=[state, state] + [small] * outer,
        ),
        out_shape=[shape, shape] + [jax.ShapeDtypeStruct((strip, span), bf16)] * outer,
        input_output_aliases={outer + 3 + i: i for i in range(len(held))},
        compiler_params=pltpu.CompilerParams(vmem_limit_bytes=24 << 20),
        cost_estimate=pl.CostEstimate(flops=8 * outer * strip * span, bytes_accessed=20 * outer * strip * span, transcendentals=0),
    )(at, *parts, weights, momentum, *held)
    return out[:2], out[2:]


def spread_kernel(outer, inner, at_ref, *refs):
    ins, outs = refs[: outer * inner], refs[outer * inner :]
    for k in range(outer):
        index = lax.rem(at_ref[1] + (outer - k), outer)
        for j in range(inner):
            outs[j][index] = ins[k * inner + j][...]


def spread(parts, at, inner):
    outer = len(parts)
    strip, span = parts[0].shape
    cols = span // inner

    def column(j):
        return pl.BlockSpec((strip, cols), lambda i, at: (0, lax.rem(at[0] + j, inner)))

    return pl.pallas_call(
        functools.partial(spread_kernel, outer, inner),
        grid_spec=pltpu.PrefetchScalarGridSpec(
            num_scalar_prefetch=1,
            grid=(1,),
            in_specs=[column(j) for _ in range(outer) for j in range(inner)],
            out_specs=[pl.BlockSpec((outer, strip, cols), lambda i, at: (0, 0, 0))] * inner,
        ),
        out_shape=[jax.ShapeDtypeStruct((outer, strip, cols), bf16)] * inner,
        compiler_params=pltpu.CompilerParams(vmem_limit_bytes=24 << 20),
        cost_estimate=pl.CostEstimate(flops=0, bytes_accessed=4 * outer * strip * span, transcendentals=0),
    )(at, *[p for p in parts for _ in range(inner)])


def write_kernel(count, low, at_ref, *refs):
    out_ref, sems = refs[-2:]
    strip = refs[0].shape[1]
    copies = []
    for i in range(count):
        target = out_ref.at[at_ref[3 * i], at_ref[3 * i + 1], :, at_ref[3 * i + 2], pl.ds(low, strip), :]
        copies.append(pltpu.make_async_copy(refs[i], target, sems.at[i]))
        copies[-1].start()
    for copy in copies:
        copy.wait()


def write(found, at, held, shape, low):
    small = pl.BlockSpec(found[0].shape, lambda i, at: (0, 0, 0))
    more = [] if held is None else [held]
    return pl.pallas_call(
        functools.partial(write_kernel, len(found), low),
        grid_spec=pltpu.PrefetchScalarGridSpec(
            num_scalar_prefetch=1,
            grid=(1,),
            in_specs=[small] * len(found) + [pl.BlockSpec(memory_space=pl.ANY) for _ in more],
            out_specs=pl.BlockSpec(memory_space=pltpu.HBM),
            scratch_shapes=[pltpu.SemaphoreType.DMA((len(found),))],
        ),
        out_shape=jax.ShapeDtypeStruct(shape, bf16),
        input_output_aliases={1 + len(found) + i: i for i in range(len(more))},
        compiler_params=pltpu.CompilerParams(vmem_limit_bytes=24 << 20),
        cost_estimate=pl.CostEstimate(flops=0, bytes_accessed=4 * len(found) * found[0].size, transcendentals=0),
    )(at, *found, *more)


def add_kernel(high, here_ref, away_ref, *out_refs):
    for j in range(1, high):

        @pl.when(pl.program_id(0) == j - 1)
        def _(j=j):
            out_refs[j - 1][...] = (here_ref[...] + away_ref[...].astype(f32)).astype(bf16)


def chip_sum(here, away, high):
    m, width = here.shape
    block = pl.BlockSpec((m // high, width // 2), lambda j, i: (j + 1, i))
    return pl.pallas_call(
        functools.partial(add_kernel, high),
        grid=(high - 1, 2),
        in_specs=[block, block],
        out_specs=[
            pl.BlockSpec((m // high, width // 2), lambda j, i, k=k: (0, jnp.where(j == k, i, jnp.where(j < k, 0, 1)))) for k in range(high - 1)
        ],
        out_shape=[jax.ShapeDtypeStruct((m // high, width), bf16) for _ in range(high - 1)],
        compiler_params=pltpu.CompilerParams(vmem_limit_bytes=24 << 20),
        cost_estimate=pl.CostEstimate(flops=m * width, bytes_accessed=8 * m * width * (high - 1) // high, transcendentals=0),
    )(here, away)


def total_kernel(outer, inner, strip, at_ref, here_ref, away_ref, *refs):
    outs = refs[-outer:]
    drifts = refs[-outer - inner : -outer]
    got = refs[: -outer - inner]
    cols = here_ref.shape[1] // inner
    for k in range(outer):
        index = lax.rem(at_ref[1] + k, outer)
        at_rows = pl.ds(pl.multiple_of(index * strip, strip), strip)
        for j in range(inner):
            at_cols = pl.ds(pl.multiple_of(lax.rem(at_ref[0] + (inner - j), inner) * cols, cols), cols)
            total = here_ref[at_rows, at_cols] + away_ref[at_rows, at_cols].astype(f32) + drifts[j][index].astype(f32)
            for ref in got:
                total = total + ref[at_rows, at_cols].astype(f32)
            outs[k][:, at_cols] = total.astype(bf16)


def full_sum(here, away, got, drifts, at, outer, low, strip):
    inner = len(drifts)
    cols = drifts[0].shape[2]
    span = inner * cols
    rows = pl.BlockSpec((outer * strip, span), lambda i, at: (0, 0))
    return pl.pallas_call(
        functools.partial(total_kernel, outer, inner, strip),
        grid_spec=pltpu.PrefetchScalarGridSpec(
            num_scalar_prefetch=1,
            grid=(1,),
            in_specs=[rows] * (2 + len(got)) + [pl.BlockSpec((outer, strip, cols), lambda i, at: (0, low // strip, 0)) for _ in drifts],
            out_specs=[pl.BlockSpec((strip, span), lambda i, at: (0, 0))] * outer,
        ),
        out_shape=[jax.ShapeDtypeStruct((strip, span), bf16)] * outer,
        compiler_params=pltpu.CompilerParams(vmem_limit_bytes=24 << 20),
        cost_estimate=pl.CostEstimate(flops=4 * outer * strip * span, bytes_accessed=12 * outer * strip * span, transcendentals=0),
    )(at, here, away, *got, *drifts)


def take_kernel(at_ref, in_ref, out_ref):
    out_ref[...] = in_ref[...]


def take(array, at, count):
    _, rows, cols = array.shape
    return pl.pallas_call(
        take_kernel,
        grid_spec=pltpu.PrefetchScalarGridSpec(
            num_scalar_prefetch=1,
            grid=(count, 2),
            in_specs=[pl.BlockSpec((1, rows // 2, cols), lambda j, i, at: (at[j], i, 0))],
            out_specs=pl.BlockSpec((1, rows // 2, cols), lambda j, i, at: (j, i, 0)),
        ),
        out_shape=jax.ShapeDtypeStruct((count, rows, cols), array.dtype),
        compiler_params=pltpu.CompilerParams(vmem_limit_bytes=24 << 20),
        cost_estimate=pl.CostEstimate(flops=0, bytes_accessed=4 * count * rows * cols, transcendentals=0),
    )(at, array)


def twin_kernel(count, at_ref, mine_ref, got_ref, *out_refs):
    for j in range(count):

        @pl.when(pl.program_id(0) == j)
        def _(j=j):
            out_refs[j][...] = (mine_ref[0].astype(f32) + got_ref[0].astype(f32)).astype(bf16)


def twin_sum(mine, got, at):
    count, rows, cols = got.shape
    count -= 1
    return pl.pallas_call(
        functools.partial(twin_kernel, count),
        grid_spec=pltpu.PrefetchScalarGridSpec(
            num_scalar_prefetch=1,
            grid=(count, 2),
            in_specs=[
                pl.BlockSpec((1, rows // 2, cols), lambda j, i, at: (at[j + 1], i, 0)),
                pl.BlockSpec((1, rows // 2, cols), lambda j, i, at: (j + 1, i, 0)),
            ],
            out_specs=[
                pl.BlockSpec((rows // 2, cols), lambda j, i, at, k=k: (jnp.where(j == k, i, jnp.where(j < k, 0, 1)), 0)) for k in range(count)
            ],
        ),
        out_shape=[jax.ShapeDtypeStruct((rows, cols), bf16) for _ in range(count)],
        compiler_params=pltpu.CompilerParams(vmem_limit_bytes=24 << 20),
        cost_estimate=pl.CostEstimate(flops=count * rows * cols, bytes_accessed=6 * count * rows * cols, transcendentals=0),
    )(at, mine, got)


def drift_kernel(inner, at_ref, *refs):
    outs, ins = refs[-inner:], refs[:-inner]
    total = ins[0][0].astype(f32) + ins[1][0].astype(f32)
    for ref in ins[2:]:
        total = total + ref[...].astype(f32)
    for j in range(inner):

        @pl.when(pl.program_id(0) == j)
        def _(j=j):
            outs[j][0] = total.astype(bf16)


def drift_sum(mine, got, more, at, place, inner, outer):
    _, length, cols = mine.shape
    rows = length // (inner * outer)

    def part(j, i, ref):
        return i * inner + lax.rem(ref[0] + j, inner)

    return pl.pallas_call(
        functools.partial(drift_kernel, inner),
        grid_spec=pltpu.PrefetchScalarGridSpec(
            num_scalar_prefetch=1,
            grid=(inner, outer),
            in_specs=[
                pl.BlockSpec((1, rows, cols), lambda j, i, ref: (ref[2], part(j, i, ref), 0)),
                pl.BlockSpec((1, rows, cols), lambda j, i, ref: (0, part(j, i, ref), 0)),
            ]
            + [pl.BlockSpec((rows, cols), lambda j, i, ref: (part(j, i, ref), 0)) for _ in more],
            out_specs=[
                pl.BlockSpec((1, rows, cols), lambda j, i, ref, k=k: (jnp.where(j == k, i, jnp.where(j < k, 0, outer - 1)), 0, 0))
                for k in range(inner)
            ],
        ),
        out_shape=[jax.ShapeDtypeStruct((outer, rows, cols), bf16) for _ in range(inner)],
        compiler_params=pltpu.CompilerParams(vmem_limit_bytes=24 << 20),
        cost_estimate=pl.CostEstimate(flops=3 * length * cols, bytes_accessed=8 * length * cols, transcendentals=0),
    )(jnp.concatenate([place, at[:1]]), mine, got, *more)


def on_device(activations, cotangent, drift, outer_weights, momentum):
    reps, tps = lax.axis_size("rep"), lax.axis_size("tp")
    inner = 2 ** (int(math.log2(tps)) // 2)
    outer = tps // inner
    pair = 2
    high = reps // pair
    rep, tp = lax.axis_index("rep"), lax.axis_index("tp")
    z, x = lax.div(tp, inner), lax.rem(tp, inner)
    y, c = lax.div(rep, pair), lax.rem(rep, pair)

    def over_x(v, k):
        return lax.ppermute(v, "tp", [(a * inner + b, a * inner + (b + k) % inner) for a in range(outer) for b in range(inner)])

    def over_z(v, k):
        return lax.ppermute(v, "tp", [(a * inner + b, (a + k) % outer * inner + b) for a in range(outer) for b in range(inner)])

    def over_y(v, k):
        return lax.ppermute(v, "rep", [(a * pair + b, (a + k) % high * pair + b) for a in range(high) for b in range(pair)])

    def over_c(v):
        return lax.ppermute(v, "rep", [(a, a ^ 1) for a in range(reps)])

    def ahead(index, k, n):
        return lax.rem(index + k, n)

    acts, cot = activations[0], cotangent[0]
    _, width = acts.shape
    cols = cot.shape[1]
    rows = outer_weights.shape[0]
    strips = cut(rows)
    n = len(strips)

    order = [ahead(y, jy, high) * pair + (c ^ jc) for jc in range(pair) for jy in range(high)]
    at = jnp.stack([x, *order]).astype(jnp.int32)
    place = jnp.stack([x, z]).astype(jnp.int32)
    own = sort_columns(acts, at, inner, outer, rows, strips)
    ring = [[own[q]] for q in range(n)]
    for q in range(n):
        for k in range(1, inner):
            ring[q].append(over_x(own[k * n + q], k))
    cots = [cot]
    for k in range(1, inner):
        cots.append(over_x(cot, k))
    for _ in range(1, outer):
        for q in range(n):
            for _ in range(inner):
                ring[q].append(over_z(ring[q][-inner], 1))

    mine = drift[0].reshape(reps, tps * rows, cols)
    near = jnp.stack(order[:high]).astype(jnp.int32)
    got = take(mine, near ^ 1, high)
    got = over_c(got)
    more = list(twin_sum(mine, got, near))
    for k in range(1, high):
        more[k - 1] = over_y(more[k - 1], k)
    drifts = list(drift_sum(mine, got, more, near, place, inner, outer))
    for k in range(1, inner):
        drifts[k] = over_x(drifts[k], k)

    weights, held = None, ()
    for q, (low, strip) in enumerate(strips):
        if q == 0:
            early = partial_grad(ring[q], cots[:1], place, outer)
            away, here = partial_grad(ring[q], cots[1:], place, outer, 1, early)
        else:
            away, here = partial_grad(ring[q], cots, place, outer)
        away = over_c(away)
        sent = chip_sum(here, away, high)
        got = []
        for j in range(1, high):
            got.append(over_y(sent[j - 1], j))
        parts = list(full_sum(here, away, got, drifts, place, outer, low, strip))
        for k in range(1, outer):
            parts[k] = over_z(parts[k], k)
        held, parts = outer_step(parts, outer_weights, momentum, held, place, low, reps)
        parts = list(parts)
        for k in range(1, outer):
            parts[k] = over_z(parts[k], outer - k)
        parts = list(spread(parts[:1] + parts[:0:-1], place, inner))
        for k in range(1, inner):
            parts[k] = over_x(parts[k], k)
        found, target = [], []
        for j in range(high):
            for k in range(inner):
                near = parts[k]
                if j > 0:
                    near = over_y(near, j)
                far = over_c(near)
                found += [near, far]
                for there in (c, c ^ 1):
                    target += [ahead(y, high - j, high), there, ahead(x, inner - k, inner)]
        weights = write(found, jnp.stack(target).astype(jnp.int32), weights, (high, pair, outer, inner, rows, cols), low)
    return (weights.reshape(width, cols), *held)


def solution(mesh):
    in_specs = (
        P("rep", "tp", None),
        P("rep", None, "tp"),
        P("rep", None, "tp"),
        P(("rep", "tp"), None),
        P(("rep", "tp"), None),
    )
    out_specs = (P(None, "tp"), P(("rep", "tp"), None), P(("rep", "tp"), None))

    return jax.shard_map(on_device, mesh=mesh, in_specs=in_specs, out_specs=out_specs, check_vma=False)
```
